32 devices in a mesh: dp: 8 (over y, x, core), tensor: 4 (over z).
Axes of the slice: x: 2, y: 2, z: 4, core: 2. Of those that a mesh axis runs over, the one named last changes fastest.
Arguments:
- inputs: bfloat16 [16, 1024, 1024], P('dp', 'tensor'), may hold values from -6 to 6
- time_vectors: float32 [16, 256], P('dp'), may hold values from -6 to 6
- segments: int32 [16, 1024], P('dp'), may hold values from 0 to 7, never falling along the last dimension, each value on 1 to 512 neighbouring positions
- attend_weight: bfloat16 [3, 1024, 1024], P(None, 'dp', 'tensor'), may hold values from -0.1875 to 0.1875
- merge_weight: bfloat16 [1024, 1024], P('tensor', 'dp'), may hold values from -0.75 to 0.75
- expand_weight: bfloat16 [1024, 4096], P('dp', 'tensor'), may hold values from -0.1875 to 0.1875
- contract_weight: bfloat16 [4096, 1024], P('tensor', 'dp'), may hold values from -0.09375 to 0.09375
- timescale_weight: bfloat16 [2, 256, 1024], P(None, None, ('dp', 'tensor')), may hold values from -0.1875 to 0.1875
- cotangent: bfloat16 [16, 1024, 1024], P('dp', 'tensor'), may hold values from -6 to 6
Outputs:
- outputs: bfloat16 [16, 1024, 1024], P('dp', 'tensor')
- grad_inputs: float32 [16, 1024, 1024], P('dp', 'tensor')
- grad_attend: float32 [3, 1024, 1024], P(None, 'dp', 'tensor')
- grad_merge: float32 [1024, 1024], P('tensor', 'dp')
- grad_expand: float32 [1024, 4096], P('dp', 'tensor')
- grad_contract: float32 [4096, 1024], P('tensor', 'dp')
- grad_timescale: float32 [2, 256, 1024], P(None, None, ('dp', 'tensor'))
The draws below stay inside these ranges and needn't reach their ends.
Inputs may be any that keep to these rules, and one draw needn't show every extreme that they name: `segments`: within each sequence segment numbers never fall; each of its 8 documents has 1 to 512 tokens, and one has exactly 512.
All inputs are finite; a program needn't handle non-finite values.
Results may differ from the reference program's by a relative error of at most 0.018.
Values may be sent and summed in bfloat16 or wider, within the bound.
A program may use at most 192 MiB of HBM per device.

```python
import math
import jax
import jax.numpy as jnp
import numpy as np
from jax import lax

D = 1024
HEADS = 16
HD = 64
FF = 4096
TDIM = 256
LEN = 1024
SEQS = 16


def with_spikes(array, own_key, source, target, blocks, factor):
    def block_of(dim):
        return (jnp.arange(array.shape[dim]) // (array.shape[dim] // blocks)).reshape((-1,) + (1,) * (array.ndim - 1 - dim))

    one_side = jax.random.permutation(own_key, blocks)[block_of(target)]
    far = (block_of(target) + blocks // 2) % blocks
    return jnp.where((block_of(source) == one_side) | (block_of(source) == far), factor * array, array)


def shard_levels(own_key, dims, cuts, smallest, largest):
    gain = 1.0
    for position, shards_of in cuts:
        draws = jax.random.uniform(jax.random.fold_in(jax.random.fold_in(own_key, 6), position), (shards_of,), jnp.float32, smallest / len(cuts), largest / len(cuts))
        gain = gain * jnp.repeat(jnp.exp(draws), dims[position] // shards_of).reshape((-1,) + (1,) * (len(dims) - 1 - position))
    return gain


def split_up(amount, total, limit, lean):
    loads = [(1 << 20) // math.isqrt(rank ** lean) + 1 for rank in range(2, amount + 1)]
    spare, given = total - limit - (amount - 1), [1] * (amount - 1)
    while spare > 0:
        candidates = [i for i in range(amount - 1) if given[i] < limit]
        pool, remaining = sum([loads[i] for i in candidates]), spare
        for i in candidates:
            extra = min(limit - given[i], max(1, remaining * loads[i] // pool), spare)
            given[i] = given[i] + extra
            spare = spare - extra
    return np.array([limit] + given)


def ragged_sizes(key, amount, total, most, slope):
    if amount == 2:
        one = jax.random.randint(key, (), max(1, total - most), min(most, total - 1) + 1)
        return jnp.stack([one, total - one])
    lengths = jnp.asarray(split_up(amount, total, most, slope), jnp.int32)
    twos = (amount - 1) // 2
    donor, taker = lengths[1:1 + 2 * twos:2], lengths[2:2 + 2 * twos:2]
    room = jnp.minimum(donor - 1, most - taker)
    passed = jax.random.randint(jax.random.fold_in(key, 1), (twos,), 0, 1 << 20) % (room + 1)
    lengths = lengths.at[1:1 + 2 * twos:2].set(donor - passed).at[2:2 + 2 * twos:2].set(taker + passed)
    return lengths[jax.random.permutation(jax.random.fold_in(key, 2), amount)]


def scatter_about(own_key, shape, width, bound, cuts=(), held_as=jnp.bfloat16):
    values = jax.random.normal(own_key, shape, jnp.float32) * width
    if len(cuts) > 0:
        values = shard_levels(own_key, shape, cuts, -0.22, 0.18) * values
    return jnp.clip(values, min=-bound, max=bound).astype(held_as)


def heavy_noise(rng, extent, scale, bound, split, heavy, held_as=jnp.bfloat16):
    values = scale * jax.random.normal(rng, extent, jnp.float32)
    if split:
        values = values * shard_levels(rng, extent, split, -0.22, 0.18)
    return jnp.clip(with_spikes(values, jax.random.fold_in(rng, 3), *heavy), -bound, bound).astype(held_as)


def setup_inputs(seed: int = 0) -> dict:
    arg_keys = jax.random.split(jax.random.key(seed), 10)
    inputs = heavy_noise(arg_keys[0], (SEQS, LEN, D), 1.0, 6.0, ((0, 8), (1, 4)), (0, 2, 8, 2.0))
    time_vectors = scatter_about(arg_keys[1], (SEQS, TDIM), 1.0, 6.0, ((0, 8),), jnp.float32)
    segments = jax.vmap(lambda own: jnp.searchsorted(jnp.cumsum(ragged_sizes(own, 8, LEN, LEN // 2, 2)), jnp.arange(LEN), side="right"))(jax.random.split(arg_keys[2], SEQS)).reshape((SEQS, LEN)).astype(jnp.int32)
    attend_weight = scatter_about(arg_keys[3], (3, D, D), D ** -0.5, 0.1875, ((1, 8), (2, 4)))
    merge_weight = scatter_about(arg_keys[4], (D, D), (D // 16) ** -0.5, 0.75, ((0, 4), (1, 8)))
    expand_weight = scatter_about(arg_keys[5], (D, FF), D ** -0.5, 0.1875, ((0, 8), (1, 4)))
    contract_weight = scatter_about(arg_keys[6], (FF, D), FF ** -0.5, 0.09375, ((0, 4), (1, 8)))
    timescale_weight = scatter_about(arg_keys[7], (2, TDIM, D), (4 * TDIM) ** -0.5, 0.1875, ((2, 32),))
    cotangent = heavy_noise(arg_keys[8], (SEQS, LEN, D), 1.0, 6.0, ((0, 8), (1, 4)), (0, 2, 8, 2.0))
    return {"inputs": inputs, "time_vectors": time_vectors, "segments": segments, "attend_weight": attend_weight, "merge_weight": merge_weight, "expand_weight": expand_weight, "contract_weight": contract_weight, "timescale_weight": timescale_weight, "cotangent": cotangent}


EPSILON = 1e-05

@jax.custom_vjp
def low(v):
    return lax.optimization_barrier(v.astype(jnp.bfloat16)).astype(jnp.float32)

@jax.custom_vjp
def low_back(v):
    return v

def low_keep(v):
    return (low(v), None)

def low_pass(kept, grad):
    return (grad,)

def back_keep(v):
    return (v, None)

def back_low(kept, grad):
    return (low(grad),)
low.defvjp(low_keep, low_pass)
low_back.defvjp(back_keep, back_low)

def normalize(values):
    center = values - lax.optimization_barrier(jnp.mean(values, axis=-1, keepdims=True))
    spread_sq = lax.optimization_barrier(jnp.mean(center * center, axis=-1, keepdims=True))
    return center * lax.rsqrt(spread_sq + EPSILON)

def one_sequence(seq_inputs, seq_time, seq_segments, attend_f, merge_f, expand_f, contract_f, timescale_f):
    highest = lax.Precision.HIGHEST
    scales = 1.0 + jnp.einsum('t,ktd->kd', seq_time, timescale_f, precision=highest)
    normed_one = low(normalize(seq_inputs) * scales[0])
    projected = low_back(low(jnp.einsum('ld,kde->kle', normed_one, attend_f, precision=highest)))
    shaped = projected.reshape(3, LEN, HEADS, HD)
    scores = low_back(jnp.einsum('qhe,khe->hqk', shaped[0], shaped[1], precision=highest) * HD ** (-0.5))
    allowed = seq_segments[:, None] == seq_segments[None, :]
    scores = jnp.where(allowed[None], scores, -1e+30)
    exponent = jnp.exp(scores - lax.optimization_barrier(jnp.max(scores, axis=-1, keepdims=True)))
    probability = exponent / lax.optimization_barrier(jnp.sum(exponent, axis=-1, keepdims=True))
    attention_result = low_back(low(jnp.einsum('hqk,khe->qhe', low(probability), shaped[2], precision=highest)))
    attention_result = attention_result.reshape(LEN, HEADS * HD)
    middle = seq_inputs + low_back(jnp.dot(attention_result, merge_f, precision=highest))
    normed_two = low(normalize(middle) * scales[1])
    hidden_pre = low_back(jnp.dot(normed_two, expand_f, precision=highest))
    hidden_activation = low(jax.nn.gelu(hidden_pre, approximate=False))
    return middle + low_back(jnp.dot(hidden_activation, contract_f, precision=highest))

def reference(inputs, time_vectors, segments, attend_weight, merge_weight, expand_weight, contract_weight, timescale_weight, cotangent):
    checked = jax.checkpoint(one_sequence)

    def forward(inputs_f, attend_f, merge_f, expand_f, contract_f, timescale_f):

        def advance(state_carry, pieces):
            return (state_carry, checked(pieces[0], pieces[1], pieces[2], attend_f, merge_f, expand_f, contract_f, timescale_f))
        _, result = lax.scan(advance, jnp.zeros((), jnp.float32), (inputs_f, time_vectors, segments))
        return result
    result, backward = jax.vjp(forward, inputs.astype(jnp.float32), attend_weight.astype(jnp.float32), merge_weight.astype(jnp.float32), expand_weight.astype(jnp.float32), contract_weight.astype(jnp.float32), timescale_weight.astype(jnp.float32))
    gradients = backward(cotangent.astype(jnp.float32))
    return (result.astype(jnp.bfloat16), gradients[0], gradients[1], gradients[2], gradients[3], gradients[4], gradients[5])
```

```python
import jax
import jax.numpy as jnp
from jax import lax
from jax.sharding import Mesh, PartitionSpec as P

HD = 64
EPSILON = 1e-05
F32 = jnp.float32
BF16 = jnp.bfloat16
HIGHEST = lax.Precision.HIGHEST


def dot(left, right, dims):
    return lax.dot_general(left, right, (dims, ((), ())), preferred_element_type=F32)


def matmul(left, right):
    return dot(left, right, ((1,), (0,)))


def matmul_nt(left, right):
    return dot(left, right, ((1,), (1,)))


def matmul_tn(left, right):
    return dot(left, right, ((0,), (0,)))


def normalize(values):
    center = values - jnp.mean(values, axis=-1, keepdims=True)
    spread_sq = jnp.mean(center * center, axis=-1, keepdims=True)
    inverse = lax.rsqrt(spread_sq + EPSILON)
    return center * inverse, inverse


def norm_back(values, scale_row, incoming):
    normed, inverse = normalize(values)
    scaled = incoming * scale_row
    mean_one = jnp.mean(scaled, axis=-1, keepdims=True)
    mean_two = jnp.mean(scaled * normed, axis=-1, keepdims=True)
    grad = inverse * (scaled - mean_one - normed * mean_two)
    return grad, jnp.sum(incoming * normed, axis=0)


def swap(value, axis):
    return lax.ppermute(value, axis, [(0, 1), (1, 0)])


def from_ahead(value, axis, step):
    size = lax.axis_size(axis)
    return lax.ppermute(value, axis, [(i, (i - step) % size) for i in range(size)])


def pick(flag, when_set, otherwise):
    return jnp.where(flag == 1, when_set, otherwise)


def pair(flag, mine, other, axis):
    return pick(
        flag,
        jnp.concatenate([other, mine], axis=axis),
        jnp.concatenate([mine, other], axis=axis),
    )


class Plane:
    def __init__(self):
        self.size = lax.axis_size("a") * lax.axis_size("b")
        self.square = lax.axis_size("a") == 2 and lax.axis_size("b") == 2

    def reorder(self, value, axis):
        if not self.square:
            return value
        axis = axis % value.ndim
        quarter = value.shape[axis] // 4
        parts = [lax.slice_in_dim(value, i * quarter, (i + 1) * quarter, axis=axis) for i in range(4)]
        flag_a, flag_b = lax.axis_index("a"), lax.axis_index("b")
        parts = [pick(flag_b, parts[i ^ 1], parts[i]) for i in range(4)]
        parts = [pick(flag_a, parts[i ^ 2], parts[i]) for i in range(4)]
        return jnp.concatenate(parts, axis=axis)

    def gather_small(self, value):
        if not self.square:
            return lax.all_gather(value, ("a", "b"))
        parts = [
            value,
            swap(value, "b"),
            swap(value, "a"),
            lax.ppermute(value, ("a", "b"), [(i, 3 - i) for i in range(4)]),
        ]
        return self.reorder(jnp.stack(parts), 0)

    def gather(self, first, second):
        if not self.square:
            return tuple(
                [lax.all_gather(half, ("a", "b"), axis=0, tiled=True)] for half in (first, second)
            )
        first_b = swap(first, "b")
        first_a = swap(jnp.stack([first, first_b]), "a")
        second_a = swap(second, "a")
        second_b = swap(jnp.stack([second, second_a]), "b")
        return (
            [first, first_b, first_a[0], first_a[1]],
            [second, second_b[0], second_a, second_b[1]],
        )

    def scatter(self, first, second):
        if not self.square:
            return tuple(
                lax.psum_scatter(half, ("a", "b"), scatter_dimension=0, tiled=True).astype(F32)
                for half in (first, second)
            )
        rows = first.shape[0] // 4
        f = [first[i * rows : (i + 1) * rows] for i in range(4)]
        s = [second[i * rows : (i + 1) * rows] for i in range(4)]
        got_f = swap(jnp.stack([f[1], f[3]]), "b").astype(F32)
        got_s = swap(jnp.stack([s[2], s[3]]), "a").astype(F32)
        late_f = swap((f[2].astype(F32) + got_f[1]).astype(BF16), "a")
        late_s = swap((s[1].astype(F32) + got_s[1]).astype(BF16), "b")
        return (
            f[0].astype(F32) + got_f[0] + late_f.astype(F32),
            s[0].astype(F32) + got_s[0] + late_s.astype(F32),
        )


def gather_weights(plane, halves):
    core = lax.axis_index("c")
    keep = pick(core, halves[1], halves[0])
    give = pick(core, halves[0], halves[1])
    own = pair(core, keep, swap(give, "c"), 0)
    line = [own] + [from_ahead(own, "t", k) for k in range(1, lax.axis_size("t"))]
    middle = len(line) // 2
    return plane.gather(
        jnp.concatenate(line[:middle], axis=1), jnp.concatenate(line[middle:], axis=1)
    )


def scatter_grads(plane, first, second):
    first, second = plane.scatter(first, second)
    count = lax.axis_size("t")
    width = first.shape[1] // (count // 2)
    pieces = [
        half[:, k * width : (k + 1) * width] for half in (first, second) for k in range(count // 2)
    ]
    total = pieces[0]
    for k in range(1, count):
        total = total + from_ahead(pieces[k].astype(BF16), "t", count - k).astype(F32)
    rows = total.shape[0] // 2
    core = lax.axis_index("c")
    keep = pick(core, total[rows:], total[:rows])
    give = pick(core, total[:rows], total[rows:])
    return pair(core, keep[None], swap(give, "c")[None], 0)


def chip_routes(count, turn):
    routes = []
    for core in range(2):
        for line in range(count):
            target = (line // 2) * count + 2 * core + (turn ^ (line % 2))
            routes.append((core * count + line, target))
    return routes


def to_chips(blocks):
    count = lax.axis_size("t")
    odd = lax.axis_index("t") % 2
    got = []
    for turn in range(2):
        give = pick(odd, blocks[1 - turn], blocks[turn])
        got.append(lax.ppermute(give, ("c", "t"), chip_routes(count, turn)))
    return pair(odd, got[0], got[1], 0)


def from_chips(rows):
    count = lax.axis_size("t")
    odd = lax.axis_index("t") % 2
    half = rows.shape[0] // 2
    got = []
    for turn in range(2):
        give = pick(odd, rows[(1 - turn) * half :][:half], rows[turn * half :][:half])
        back = [(target, source) for source, target in chip_routes(count, turn)]
        got.append(lax.ppermute(give, ("c", "t"), back))
    return pair(odd, got[0][None], got[1][None], 0)


def both(mine):
    return jnp.concatenate([mine, swap(mine, "c")], axis=0)


def settle(partial):
    half = partial.shape[0] // 2
    return partial[:half] + swap(partial[half:].astype(BF16), "c").astype(F32)


def attend_forward(projected, segment):
    length = projected.shape[0]
    shaped = projected.reshape(length, -1, 3, 2, HD)
    query, keys, values = shaped[:, :, 0], shaped[:, :, 1], shaped[:, :, 2]
    scores = jnp.einsum("qghe,kghe->ghqk", query, keys, preferred_element_type=F32) * HD ** (-0.5)
    allowed = segment[:, None] == segment[None, :]
    scores = jnp.where(allowed, scores, -1e30)
    highest = jnp.max(scores, axis=-1, keepdims=True)
    exponent = jnp.exp(scores - highest)
    totals = jnp.sum(exponent, axis=-1, keepdims=True)
    probability = (exponent / totals).astype(BF16)
    result = jnp.einsum("ghqk,kghe->qghe", probability, values, preferred_element_type=F32)
    return result.astype(BF16).reshape(length, -1), highest + jnp.log(totals)


def attend_backward(projected, segment, log_totals, grad_attended):
    length = projected.shape[0]
    shaped = projected.reshape(length, -1, 3, 2, HD)
    query, keys, values = shaped[:, :, 0], shaped[:, :, 1], shaped[:, :, 2]
    grad_heads = grad_attended.reshape(length, -1, 2, HD)
    scores = jnp.einsum("qghe,kghe->ghqk", query, keys, preferred_element_type=F32) * HD ** (-0.5)
    allowed = segment[:, None] == segment[None, :]
    scores = jnp.where(allowed, scores, -1e30)
    probability = jnp.exp(scores - log_totals)
    grad_prob = jnp.einsum("qghe,kghe->ghqk", grad_heads, values, preferred_element_type=F32)
    inner_sum = jnp.sum(probability * grad_prob, axis=-1, keepdims=True)
    grad_scores = (probability * (grad_prob - inner_sum)).astype(BF16)
    factor = HD ** (-0.5)
    grad_query = jnp.einsum("ghqk,kghe->qghe", grad_scores, keys, preferred_element_type=F32) * factor
    grad_keys = jnp.einsum("ghqk,qghe->kghe", grad_scores, query, preferred_element_type=F32) * factor
    grad_values = jnp.einsum(
        "ghqk,qghe->kghe", probability.astype(BF16), grad_heads, preferred_element_type=F32
    )
    return (
        jnp.stack([grad_query, grad_keys, grad_values], axis=2).astype(BF16).reshape(length, -1)
    )


def shards(
    inputs,
    time_vectors,
    segments,
    attend_weight,
    merge_weight,
    expand_weight,
    contract_weight,
    timescale_weight,
    cotangent,
):
    plane = Plane()
    core, line = lax.axis_index("c"), lax.axis_index("t")
    count = lax.axis_size("t")
    assert count == 4 and inputs.shape[0] == 2
    rows = attend_weight.shape[1]
    owner, place = line // 2, line % 2

    def chip_row(value):
        both_cores = pair(core, value[None], swap(value, "c")[None], 0)
        return pick(
            owner,
            pick(place, both_cores[1, 1], both_cores[1, 0]),
            pick(place, both_cores[0, 1], both_cores[0, 0]),
        )

    rows_in = plane.reorder(to_chips(inputs), 1)
    rows_cot = plane.reorder(to_chips(cotangent), 1)
    segment = chip_row(segments)
    half_length = segment.shape[0] // 2
    segment = pick(
        core,
        jnp.concatenate([segment[half_length:], segment[:half_length]]),
        segment,
    )

    def column_halves(matrix):
        half = matrix.shape[1] // 2
        return [matrix[:, :half], matrix[:, half:]]

    attend_parts = [column_halves(attend_weight[k]) for k in range(3)]
    merge_parts = column_halves(merge_weight.T)
    head_width = merge_parts[0].shape[1]
    first_pack = [
        jnp.concatenate([attend_parts[k][h] for k in range(3)] + [merge_parts[h]], axis=1)
        for h in range(2)
    ]
    head_pieces = gather_weights(plane, first_pack)
    expand_pieces = gather_weights(plane, column_halves(expand_weight))
    contract_pieces = gather_weights(plane, column_halves(contract_weight.T))
    line_width = 4 * head_width

    def slabs(pieces, low, high):
        columns = []
        for half in pieces:
            whole = jnp.concatenate(half, axis=0)
            for k in range(count // 2):
                columns.append(whole[:, k * line_width + low : k * line_width + high])
        return jnp.concatenate(columns, axis=1)

    attend_whole = slabs(head_pieces, 0, 3 * head_width)
    merge_whole = slabs(head_pieces, 3 * head_width, 4 * head_width)
    expand_whole = jnp.concatenate([jnp.concatenate(half, axis=0) for half in expand_pieces], axis=1)
    contract_whole = jnp.concatenate(
        [jnp.concatenate(half, axis=0) for half in contract_pieces], axis=1
    )

    times = plane.gather_small(
        pair(core, time_vectors[None], swap(time_vectors, "c")[None], 0)
    ).reshape(-1, time_vectors.shape[1])
    scale_part = 1.0 + jnp.einsum(
        "st,ktd->skd", times, timescale_weight.astype(F32), precision=HIGHEST
    )
    piece = scale_part.shape[2]
    scale_line = jnp.stack([scale_part] + [from_ahead(scale_part, "t", k) for k in range(1, count)])
    scale_line = jnp.roll(scale_line, line, axis=0)
    scale_line = pair(core, scale_line[None], swap(scale_line, "c")[None], 0)
    scale_all = plane.gather_small(scale_line)
    position = lax.axis_index("a") * lax.axis_size("b") + lax.axis_index("b")
    mine = lax.dynamic_index_in_dim(scale_all, position * count + line, axis=3, keepdims=False)
    scales = plane.reorder(jnp.moveaxis(mine, 3, 0).reshape(2, -1), 1)
    scale_one, scale_two = scales[0:1], scales[1:2]

    rows_f32 = rows_in.astype(F32)
    normed_one = both((normalize(rows_f32)[0] * scale_one).astype(BF16))
    projected = matmul(normed_one, attend_whole).astype(BF16)
    attended, log_totals = attend_forward(projected, segment)
    middle = rows_f32 + settle(matmul_nt(attended, merge_whole))
    normed_two = both((normalize(middle)[0] * scale_two).astype(BF16))
    hidden_pre = matmul(normed_two, expand_whole)
    density = 0.5 * (1.0 + lax.erf(hidden_pre * (0.5**0.5)))
    slope = (
        density + hidden_pre * jnp.exp(-0.5 * hidden_pre * hidden_pre) * 0.3989422804014327
    ).astype(BF16)
    hidden = (hidden_pre * density).astype(BF16)
    rows_out = (middle + settle(matmul_nt(hidden, contract_whole))).astype(BF16)
    outputs = from_chips(plane.reorder(rows_out, 1))

    def weight_grad(left, right):
        half = right.shape[1] // 2
        return [matmul_tn(left, part).astype(BF16) for part in (right[:, :half], right[:, half:])]

    cot_all = both(rows_cot)
    contract_grad = scatter_grads(plane, *weight_grad(cot_all, hidden))
    grad_pre = (matmul(cot_all, contract_whole) * slope.astype(F32)).astype(BF16)
    expand_grad = scatter_grads(plane, *weight_grad(normed_two, grad_pre))
    grad_normed_two = settle(matmul_nt(grad_pre, expand_whole))
    part, scale_grad_two = norm_back(middle, scale_two, grad_normed_two)
    grad_middle = rows_cot.astype(F32) + part
    grad_middle_all = both(grad_middle.astype(BF16))
    grad_attended = matmul(grad_middle_all, merge_whole).astype(BF16)
    merge_grad = matmul_tn(grad_middle_all, attended).astype(BF16)
    grad_projected = attend_backward(projected, segment, log_totals, grad_attended)
    attend_grad = matmul_tn(normed_one, grad_projected).astype(BF16)
    columns = []
    for k in range(count):
        columns.append(attend_grad[:, k * 3 * head_width : (k + 1) * 3 * head_width])
        columns.append(merge_grad[:, k * head_width : (k + 1) * head_width])
    middle_column = len(columns) // 2
    head_grad = scatter_grads(
        plane,
        jnp.concatenate(columns[:middle_column], axis=1),
        jnp.concatenate(columns[middle_column:], axis=1),
    )
    grad_normed_one = settle(matmul_nt(grad_projected, attend_whole))
    part, scale_grad_one = norm_back(rows_f32, scale_one, grad_normed_one)
    rows_grad = (grad_middle + part).astype(BF16)
    grad_inputs = from_chips(plane.reorder(rows_grad, 1)).astype(F32)

    def joined(grad):
        return jnp.concatenate([grad[0], grad[1]], axis=1)

    grad_attend = jnp.stack(
        [joined(head_grad[:, :, k * head_width : (k + 1) * head_width]) for k in range(3)]
    )
    grad_merge = joined(head_grad[:, :, 3 * head_width :]).T
    grad_expand = joined(expand_grad)
    grad_contract = joined(contract_grad).T

    scale_grad = jnp.stack([scale_grad_one, scale_grad_two])
    scale_grad = plane.reorder(scale_grad + swap(scale_grad, "c"), 1)
    scale_grad = jnp.stack([scale_grad] + [from_ahead(scale_grad, "t", k) for k in range(1, count)])
    scale_grad = plane.gather_small(jnp.roll(scale_grad, line, axis=0))
    scale_grad = scale_grad.reshape(-1, 2, scale_grad.shape[-1])
    offset = ((position * 2 + core) * count + line) * piece
    scale_grad = lax.dynamic_slice_in_dim(scale_grad, offset, piece, axis=2)
    grad_timescale = jnp.einsum("st,skd->ktd", times, scale_grad, precision=HIGHEST)
    return (
        outputs,
        grad_inputs,
        grad_attend,
        grad_merge,
        grad_expand,
        grad_contract,
        grad_timescale,
    )


def solution(mesh):
    outer, line = mesh.shape["dp"] // 4, mesh.shape["tensor"]
    grid = Mesh(mesh.devices.reshape(outer, 2, 2, line), ("a", "b", "c", "t"))
    dp = ("a", "b", "c")
    return jax.shard_map(
        shards,
        mesh=grid,
        in_specs=(
            P(dp, "t", None),
            P(dp, None),
            P(dp, None),
            P(None, dp, "t"),
            P("t", dp),
            P(dp, "t"),
            P("t", dp),
            P(None, None, dp + ("t",)),
            P(dp, "t", None),
        ),
        out_specs=(
            P(dp, "t", None),
            P(dp, "t", None),
            P(None, dp, "t"),
            P("t", dp),
            P(dp, "t"),
            P("t", dp),
            P(None, None, dp + ("t",)),
        ),
        check_vma=False,
    )
```

```python
import functools

import jax
import jax.numpy as jnp
from jax import lax
from jax.experimental import pallas as pl
from jax.experimental.pallas import tpu as pltpu
from jax.sharding import Mesh, PartitionSpec as P

HD = 64
EPSILON = 1e-05
F32 = jnp.float32
BF16 = jnp.bfloat16
HIGHEST = lax.Precision.HIGHEST


def dot(left, right, dims):
    return lax.dot_general(left, right, (dims, ((), ())), preferred_element_type=F32)


def matmul(left, right):
    return dot(left, right, ((1,), (0,)))


def matmul_nt(left, right):
    return dot(left, right, ((1,), (1,)))


def matmul_tn(left, right):
    return dot(left, right, ((0,), (0,)))


def normalize(values):
    center = values - jnp.mean(values, axis=-1, keepdims=True)
    spread_sq = jnp.mean(center * center, axis=-1, keepdims=True)
    inverse = lax.rsqrt(spread_sq + EPSILON)
    return center * inverse, inverse


def norm_back(values, scale_row, incoming):
    normed, inverse = normalize(values)
    scaled = incoming * scale_row
    mean_one = jnp.mean(scaled, axis=-1, keepdims=True)
    mean_two = jnp.mean(scaled * normed, axis=-1, keepdims=True)
    grad = inverse * (scaled - mean_one - normed * mean_two)
    return grad, jnp.sum(incoming * normed, axis=0)


def swap(value, axis):
    return lax.ppermute(value, axis, [(0, 1), (1, 0)])


def from_ahead(value, axis, step):
    size = lax.axis_size(axis)
    return lax.ppermute(value, axis, [(i, (i - step) % size) for i in range(size)])


def pick(flag, when_set, otherwise):
    return jnp.where(flag == 1, when_set, otherwise)


def pair(flag, mine, other, axis):
    return pick(
        flag,
        jnp.concatenate([other, mine], axis=axis),
        jnp.concatenate([mine, other], axis=axis),
    )


class Plane:
    def __init__(self):
        self.size = lax.axis_size("a") * lax.axis_size("b")
        self.square = lax.axis_size("a") == 2 and lax.axis_size("b") == 2

    def reorder(self, value, axis):
        if not self.square:
            return value
        axis = axis % value.ndim
        quarter = value.shape[axis] // 4
        parts = [lax.slice_in_dim(value, i * quarter, (i + 1) * quarter, axis=axis) for i in range(4)]
        flag_a, flag_b = lax.axis_index("a"), lax.axis_index("b")
        parts = [pick(flag_b, parts[i ^ 1], parts[i]) for i in range(4)]
        parts = [pick(flag_a, parts[i ^ 2], parts[i]) for i in range(4)]
        return jnp.concatenate(parts, axis=axis)

    def gather_small(self, value):
        if not self.square:
            return lax.all_gather(value, ("a", "b"))
        parts = [
            value,
            swap(value, "b"),
            swap(value, "a"),
            lax.ppermute(value, ("a", "b"), [(i, 3 - i) for i in range(4)]),
        ]
        return self.reorder(jnp.stack(parts), 0)

    def gather(self, first, second):
        if not self.square:
            return tuple(
                [lax.all_gather(half, ("a", "b"), axis=0, tiled=True)] for half in (first, second)
            )
        first_b = swap(first, "b")
        first_a = swap(jnp.stack([first, first_b]), "a")
        second_a = swap(second, "a")
        second_b = swap(jnp.stack([second, second_a]), "b")
        return (
            [first, first_b, first_a[0], first_a[1]],
            [second, second_b[0], second_a, second_b[1]],
        )

    def scatter(self, first, second):
        if not self.square:
            return tuple(
                lax.psum_scatter(half, ("a", "b"), scatter_dimension=0, tiled=True).astype(F32)
                for half in (first, second)
            )
        rows = first.shape[0] // 4
        f = [first[i * rows : (i + 1) * rows] for i in range(4)]
        s = [second[i * rows : (i + 1) * rows] for i in range(4)]
        got_f = swap(jnp.stack([f[1], f[3]]), "b").astype(F32)
        got_s = swap(jnp.stack([s[2], s[3]]), "a").astype(F32)
        late_f = swap((f[2].astype(F32) + got_f[1]).astype(BF16), "a")
        late_s = swap((s[1].astype(F32) + got_s[1]).astype(BF16), "b")
        return (
            f[0].astype(F32) + got_f[0] + late_f.astype(F32),
            s[0].astype(F32) + got_s[0] + late_s.astype(F32),
        )


def after(value, *earlier):
    return lax.optimization_barrier((value,) + earlier)[0]


def core_columns(halves):
    core = lax.axis_index("c")
    keep = pick(core, halves[1], halves[0])
    give = pick(core, halves[0], halves[1])
    return pair(core, keep, swap(give, "c"), 0)


def gather_line(own):
    line = [own] + [from_ahead(own, "t", k) for k in range(1, lax.axis_size("t"))]
    middle = len(line) // 2
    return jnp.concatenate(line[:middle], axis=1), jnp.concatenate(line[middle:], axis=1)


def scatter_grads(plane, first, second):
    first, second = plane.scatter(first, second)
    count = lax.axis_size("t")
    width = first.shape[1] // (count // 2)
    pieces = [
        half[:, k * width : (k + 1) * width] for half in (first, second) for k in range(count // 2)
    ]
    total = pieces[0]
    for k in range(1, count):
        total = total + from_ahead(pieces[k].astype(BF16), "t", count - k).astype(F32)
    rows = total.shape[0] // 2
    core = lax.axis_index("c")
    keep = pick(core, total[rows:], total[:rows])
    give = pick(core, total[:rows], total[rows:])
    return pair(core, keep[None], swap(give, "c")[None], 0)


def chip_routes(count, turn):
    routes = []
    for core in range(2):
        for line in range(count):
            target = (line // 2) * count + 2 * core + (turn ^ (line % 2))
            routes.append((core * count + line, target))
    return routes


def to_chips(blocks):
    count = lax.axis_size("t")
    odd = lax.axis_index("t") % 2
    got = []
    for turn in range(2):
        give = pick(odd, blocks[1 - turn], blocks[turn])
        got.append(lax.ppermute(give, ("c", "t"), chip_routes(count, turn)))
    return pair(odd, got[0], got[1], 0)


def from_chips(rows):
    count = lax.axis_size("t")
    odd = lax.axis_index("t") % 2
    half = rows.shape[0] // 2
    got = []
    for turn in range(2):
        give = pick(odd, rows[(1 - turn) * half :][:half], rows[turn * half :][:half])
        back = [(target, source) for source, target in chip_routes(count, turn)]
        got.append(lax.ppermute(give, ("c", "t"), back))
    return pair(odd, got[0][None], got[1][None], 0)


def both(mine):
    return jnp.concatenate([mine, swap(mine, "c")], axis=0)


def settle(partial):
    half = partial.shape[0] // 2
    return partial[:half] + swap(partial[half:].astype(BF16), "c").astype(F32)


def mask_rows(step, tile, column_ref, row_ref, mask_ref):
    @pl.when(pl.program_id(0) == 0)
    def _():
        queries = row_ref[:, pl.ds(pl.multiple_of(step * tile, tile), tile)]
        mask_ref[step] = jnp.where(column_ref[...] == queries, 0.0, -1e30)


def attend_forward_kernel(tile, column_ref, row_ref, projected_ref, out_ref, total_ref, mask_ref):
    step = pl.program_id(1)
    mask_rows(step, tile, column_ref, row_ref, mask_ref)
    rows = pl.ds(pl.multiple_of(step * tile, tile), tile)
    results = []
    for head in range(2):
        low = head * HD
        query = projected_ref[rows, low : low + HD] * HD ** (-0.5)
        keys = projected_ref[:, 2 * HD + low : 3 * HD + low]
        values = projected_ref[:, 4 * HD + low : 5 * HD + low]
        scores = dot(keys, query, ((1,), (1,))) + mask_ref[step]
        highest = jnp.max(scores, axis=0, keepdims=True)
        exponent = jnp.exp(scores - highest)
        totals = jnp.sum(exponent, axis=0, keepdims=True)
        result = dot(values, exponent.astype(BF16), ((0,), (0,))) / totals
        results.append(result)
        total_ref[0, head : head + 1, rows] = highest + jnp.log(totals)
    out_ref[rows, :] = jnp.concatenate(results, axis=0).T.astype(BF16)


def attend_backward_kernel(
    tile, column_ref, row_ref, projected_ref, grad_ref, total_ref, out_ref, mask_ref, keys_ref, values_ref
):
    step = pl.program_id(1)
    mask_rows(step, tile, column_ref, row_ref, mask_ref)
    rows = pl.ds(pl.multiple_of(step * tile, tile), tile)

    @pl.when(step == 0)
    def _():
        keys_ref[...] = jnp.zeros_like(keys_ref)
        values_ref[...] = jnp.zeros_like(values_ref)

    grads_query = []
    grads_keys = []
    grads_values = []
    for head in range(2):
        low = head * HD
        query = projected_ref[rows, low : low + HD] * HD ** (-0.5)
        keys = projected_ref[:, 2 * HD + low : 3 * HD + low]
        values = projected_ref[:, 4 * HD + low : 5 * HD + low]
        grad = grad_ref[rows, low : low + HD]
        scores = dot(keys, query, ((1,), (1,))) + mask_ref[step]
        probability = jnp.exp(scores - total_ref[0, head : head + 1, rows])
        grad_prob = dot(values, grad, ((1,), (1,)))
        inner_sum = jnp.sum(probability * grad_prob, axis=0, keepdims=True)
        grad_scores = (probability * (grad_prob - inner_sum)).astype(BF16)
        grads_values.append(dot(probability.astype(BF16), grad, ((1,), (0,))))
        grads_keys.append(dot(grad_scores, query, ((1,), (0,))))
        grads_query.append(dot(keys, grad_scores, ((0,), (0,))))
    keys_ref[...] += jnp.concatenate(grads_keys, axis=1)
    values_ref[...] += jnp.concatenate(grads_values, axis=1)
    grad_query = jnp.concatenate(grads_query, axis=0).T * HD ** (-0.5)
    out_ref[rows, 0 : 2 * HD] = grad_query.astype(BF16)

    @pl.when(step == pl.num_programs(1) - 1)
    def _():
        out_ref[:, 2 * HD : 4 * HD] = keys_ref[...].astype(BF16)
        out_ref[:, 4 * HD : 6 * HD] = values_ref[...].astype(BF16)


def attention_specs(length, tile):
    whole = lambda group, step: (0, 0)
    by_group = lambda group, step: (0, group)
    return dict(
        column=pl.BlockSpec((length, 1), whole),
        row=pl.BlockSpec((1, length), whole),
        projected=pl.BlockSpec((length, 6 * HD), by_group),
        attended=pl.BlockSpec((length, 2 * HD), by_group),
        total=pl.BlockSpec((1, 8, length), lambda group, step: (group, 0, 0)),
        mask=pltpu.VMEM((length // tile, length, tile), F32),
    )


def attend_forward(projected, segment):
    length = projected.shape[0]
    groups = projected.shape[1] // (6 * HD)
    tile = min(256, length)
    specs = attention_specs(length, tile)
    pairs = groups * 2 * length * length
    return pl.pallas_call(
        functools.partial(attend_forward_kernel, tile),
        out_shape=(
            jax.ShapeDtypeStruct((length, groups * 2 * HD), BF16),
            jax.ShapeDtypeStruct((groups, 8, length), F32),
        ),
        grid=(groups, length // tile),
        in_specs=[specs["column"], specs["row"], specs["projected"]],
        out_specs=(specs["attended"], specs["total"]),
        scratch_shapes=[specs["mask"]],
        cost_estimate=pl.CostEstimate(
            flops=16 * pairs * HD, transcendentals=pairs, bytes_accessed=8 * length * groups * 2 * HD
        ),
    )(segment[:, None], segment[None, :], projected)


def attend_backward(projected, segment, totals, grad_attended):
    length = projected.shape[0]
    groups = projected.shape[1] // (6 * HD)
    tile = min(256, length)
    specs = attention_specs(length, tile)
    pairs = groups * 2 * length * length
    return pl.pallas_call(
        functools.partial(attend_backward_kernel, tile),
        out_shape=jax.ShapeDtypeStruct(projected.shape, BF16),
        grid=(groups, length // tile),
        in_specs=[
            specs["column"],
            specs["row"],
            specs["projected"],
            specs["attended"],
            specs["total"],
        ],
        out_specs=specs["projected"],
        scratch_shapes=[
            specs["mask"],
            pltpu.VMEM((length, 2 * HD), F32),
            pltpu.VMEM((length, 2 * HD), F32),
        ],
        cost_estimate=pl.CostEstimate(
            flops=40 * pairs * HD, transcendentals=pairs, bytes_accessed=16 * length * groups * 2 * HD
        ),
    )(segment[:, None], segment[None, :], projected, grad_attended, totals)


def shards(
    inputs,
    time_vectors,
    segments,
    attend_weight,
    merge_weight,
    expand_weight,
    contract_weight,
    timescale_weight,
    cotangent,
):
    plane = Plane()
    core, line = lax.axis_index("c"), lax.axis_index("t")
    count = lax.axis_size("t")
    assert count == 4 and inputs.shape[0] == 2
    rows = attend_weight.shape[1]
    owner, place = line // 2, line % 2

    def chip_row(value):
        both_cores = pair(core, value[None], swap(value, "c")[None], 0)
        return pick(
            owner,
            pick(place, both_cores[1, 1], both_cores[1, 0]),
            pick(place, both_cores[0, 1], both_cores[0, 0]),
        )

    rows_in = plane.reorder(to_chips(inputs), 1)
    segment = chip_row(segments)
    half_length = segment.shape[0] // 2
    segment = pick(
        core,
        jnp.concatenate([segment[half_length:], segment[:half_length]]),
        segment,
    )

    def column_halves(matrix):
        half = matrix.shape[1] // 2
        return [matrix[:, :half], matrix[:, half:]]

    attend_parts = [column_halves(attend_weight[k]) for k in range(3)]
    merge_parts = column_halves(merge_weight.T)
    head_width = merge_parts[0].shape[1]
    first_pack = [
        jnp.concatenate([attend_parts[k][h] for k in range(3)] + [merge_parts[h]], axis=1)
        for h in range(2)
    ]
    head_line = gather_line(core_columns(first_pack))
    head_pieces = plane.gather(*head_line)
    expand_own = after(core_columns(column_halves(expand_weight)), rows_in, *head_line)
    expand_line = gather_line(expand_own)
    expand_pieces = plane.gather(
        after(expand_line[0], *head_pieces[0]), after(expand_line[1], *head_pieces[1])
    )
    rows_cot = plane.reorder(to_chips(after(cotangent, *expand_line)), 1)
    contract_own = after(core_columns(column_halves(contract_weight.T)), *expand_line)
    contract_line = gather_line(contract_own)
    contract_pieces = plane.gather(
        after(contract_line[0], *expand_pieces[0]), after(contract_line[1], *expand_pieces[1])
    )
    line_width = 4 * head_width

    def slabs(pieces, low, high):
        columns = []
        for half in pieces:
            whole = jnp.concatenate(half, axis=0)
            for k in range(count // 2):
                columns.append(whole[:, k * line_width + low : k * line_width + high])
        return jnp.concatenate(columns, axis=1)

    attend_whole = slabs(head_pieces, 0, 3 * head_width)
    merge_whole = slabs(head_pieces, 3 * head_width, 4 * head_width)
    expand_whole = jnp.concatenate([jnp.concatenate(half, axis=0) for half in expand_pieces], axis=1)
    contract_whole = jnp.concatenate(
        [jnp.concatenate(half, axis=0) for half in contract_pieces], axis=1
    )

    times = plane.gather_small(
        pair(core, time_vectors[None], swap(time_vectors, "c")[None], 0)
    ).reshape(-1, time_vectors.shape[1])
    scale_part = 1.0 + jnp.einsum(
        "st,ktd->skd", times, timescale_weight.astype(F32), precision=HIGHEST
    )
    piece = scale_part.shape[2]
    scale_line = jnp.stack([scale_part] + [from_ahead(scale_part, "t", k) for k in range(1, count)])
    scale_line = jnp.roll(scale_line, line, axis=0)
    scale_line = pair(core, scale_line[None], swap(scale_line, "c")[None], 0)
    scale_all = plane.gather_small(scale_line)
    position = lax.axis_index("a") * lax.axis_size("b") + lax.axis_index("b")
    mine = lax.dynamic_index_in_dim(scale_all, position * count + line, axis=3, keepdims=False)
    scales = plane.reorder(jnp.moveaxis(mine, 3, 0).reshape(2, -1), 1)
    scale_one, scale_two = scales[0:1], scales[1:2]

    rows_f32 = rows_in.astype(F32)
    normed_one = both((normalize(rows_f32)[0] * scale_one).astype(BF16))
    projected = matmul(normed_one, attend_whole).astype(BF16)
    attended, log_totals = attend_forward(projected, segment)
    middle = rows_f32 + settle(matmul_nt(attended, merge_whole))
    normed_two = both((normalize(middle)[0] * scale_two).astype(BF16))
    hidden_pre = matmul(normed_two, expand_whole)
    density = 0.5 * (1.0 + lax.erf(hidden_pre * (0.5**0.5)))
    slope = (
        density + hidden_pre * jnp.exp(-0.5 * hidden_pre * hidden_pre) * 0.3989422804014327
    ).astype(BF16)
    hidden = (hidden_pre * density).astype(BF16)
    rows_out = (middle + settle(matmul_nt(hidden, contract_whole))).astype(BF16)
    outputs = from_chips(plane.reorder(rows_out, 1))

    def weight_grad(left, right):
        half = right.shape[1] // 2
        return [matmul_tn(left, part).astype(BF16) for part in (right[:, :half], right[:, half:])]

    cot_all = both(rows_cot)
    contract_grad = scatter_grads(plane, *weight_grad(cot_all, hidden))
    grad_pre = (matmul(cot_all, contract_whole) * slope.astype(F32)).astype(BF16)
    expand_grad = scatter_grads(plane, *weight_grad(normed_two, grad_pre))
    grad_normed_two = settle(matmul_nt(grad_pre, expand_whole))
    part, scale_grad_two = norm_back(middle, scale_two, grad_normed_two)
    grad_middle = rows_cot.astype(F32) + part
    grad_middle_all = both(grad_middle.astype(BF16))
    grad_attended = matmul(grad_middle_all, merge_whole).astype(BF16)
    merge_grad = matmul_tn(grad_middle_all, attended).astype(BF16)
    grad_projected = attend_backward(projected, segment, log_totals, grad_attended)
    attend_grad = matmul_tn(normed_one, grad_projected).astype(BF16)
    columns = []
    for k in range(count):
        columns.append(attend_grad[:, k * 3 * head_width : (k + 1) * 3 * head_width])
        columns.append(merge_grad[:, k * head_width : (k + 1) * head_width])
    middle_column = len(columns) // 2
    head_grad = scatter_grads(
        plane,
        jnp.concatenate(columns[:middle_column], axis=1),
        jnp.concatenate(columns[middle_column:], axis=1),
    )
    grad_normed_one = settle(matmul_nt(grad_projected, attend_whole))
    part, scale_grad_one = norm_back(rows_f32, scale_one, grad_normed_one)
    rows_grad = (grad_middle + part).astype(BF16)
    grad_inputs = from_chips(plane.reorder(rows_grad, 1)).astype(F32)

    def joined(grad):
        return jnp.concatenate([grad[0], grad[1]], axis=1)

    grad_attend = jnp.stack(
        [joined(head_grad[:, :, k * head_width : (k + 1) * head_width]) for k in range(3)]
    )
    grad_merge = joined(head_grad[:, :, 3 * head_width :]).T
    grad_expand = joined(expand_grad)
    grad_contract = joined(contract_grad).T

    scale_grad = jnp.stack([scale_grad_one, scale_grad_two])
    scale_grad = plane.reorder(scale_grad + swap(scale_grad, "c"), 1)
    scale_grad = jnp.stack([scale_grad] + [from_ahead(scale_grad, "t", k) for k in range(1, count)])
    scale_grad = plane.gather_small(jnp.roll(scale_grad, line, axis=0))
    scale_grad = scale_grad.reshape(-1, 2, scale_grad.shape[-1])
    offset = ((position * 2 + core) * count + line) * piece
    scale_grad = lax.dynamic_slice_in_dim(scale_grad, offset, piece, axis=2)
    grad_timescale = jnp.einsum("st,skd->ktd", times, scale_grad, precision=HIGHEST)
    return (
        outputs,
        grad_inputs,
        grad_attend,
        grad_merge,
        grad_expand,
        grad_contract,
        grad_timescale,
    )


def solution(mesh):
    outer, line = mesh.shape["dp"] // 4, mesh.shape["tensor"]
    grid = Mesh(mesh.devices.reshape(outer, 2, 2, line), ("a", "b", "c", "t"))
    dp = ("a", "b", "c")
    return jax.shard_map(
        shards,
        mesh=grid,
        in_specs=(
            P(dp, "t", None),
            P(dp, None),
            P(dp, None),
            P(None, dp, "t"),
            P("t", dp),
            P(dp, "t"),
            P("t", dp),
            P(None, None, dp + ("t",)),
            P(dp, "t", None),
        ),
        out_specs=(
            P(dp, "t", None),
            P(dp, "t", None),
            P(None, dp, "t"),
            P("t", dp),
            P(dp, "t"),
            P("t", dp),
            P(None, None, dp + ("t",)),
        ),
        check_vma=False,
    )
```
